32 devices in a mesh: dp: 4 (over x, core), expert: 8 (over z, y).
Axes of the slice: x: 2, y: 2, z: 4, core: 2. Of those that a mesh axis runs over, the one named last changes fastest.
Arguments:
- tokens: bfloat16 [4096, 1024], P(('dp', 'expert')), may hold values from -6 to 6
- cotangent: bfloat16 [4096, 1024], P(('dp', 'expert')), may hold values from -6 to 6
- routing: int32 [4096, 2], P(('dp', 'expert')), may hold values from 0 to 7, all different within a row; in each aligned block of 128 rows (0 to 127, 128 to 255, ...) at most 64 rows name the same one
- gate_values: float32 [4096, 2], P(('dp', 'expert')), may hold values from 0.1 to 1
- live_counts: int32 [32], P(('dp', 'expert')), may hold values from 64 to 128
- gate_weights: bfloat16 [8, 1024, 384], P('expert', 'dp'), may hold values from -0.1875 to 0.1875
- up_weights: bfloat16 [8, 1024, 384], P('expert', 'dp'), may hold values from -0.1875 to 0.1875
- down_weights: bfloat16 [8, 384, 1024], P('expert', 'dp'), may hold values from -0.3125 to 0.3125
Outputs:
- mixed: bfloat16 [4096, 1024], P(('dp', 'expert'))
- token_grad: bfloat16 [4096, 1024], P(('dp', 'expert'))
- gate_grad: float32 [4096, 2], P(('dp', 'expert'))
- grad_gate_w: bfloat16 [8, 1024, 384], P('expert', 'dp')
- grad_up_w: bfloat16 [8, 1024, 384], P('expert', 'dp')
- grad_down_w: bfloat16 [8, 384, 1024], P('expert', 'dp')
The draws below stay inside these ranges and needn't reach their ends.
Inputs may be any that keep to these rules, and one draw needn't show every extreme that they name: `routing`: each row names 2 different experts; among the 128 rows of one device no expert is named by more than 64 rows.
All inputs are finite; a program needn't handle non-finite values.
Results may differ from the reference program's by a relative error of at most 0.018.
Values may be sent and summed in bfloat16 or wider, within the bound.
No kernel may reach another device: no remote copies, remote signals or barrier semaphores. Data moves between devices by JAX's collectives and lax.ppermute only.
A program may use at most 64 MiB of HBM per device.

```python
import math
import jax
import jax.numpy as jnp
import numpy as np
from jax import lax

D = 1024
FF = 384
TOP = 2
TOK_DEV = 128
EXPERTS = 8
CAP = 64
GROUPS = 4
TOKENS = 4096
N_EXPERT = 8
DEVICES = 32


def place_ends(values, key, low, top_value):
    longest = values.shape.index(max(values.shape))
    spots = []
    for shift in (0, 1):
        where = [jax.random.randint(jax.random.fold_in(key, axis), (), 0, length) for axis, length in enumerate(values.shape)]
        where[longest] = (where[longest] + shift) % values.shape[longest]
        spots.append(tuple(where))
    return values.at[spots[0]].set(low).at[spots[1]].set(top_value)


def block_scale(stream_key, dims, split, low, high):
    factor_of = 1.0
    for position, blocks in split:
        heights = jax.random.uniform(jax.random.fold_in(jax.random.fold_in(stream_key, 6), position), (blocks,), jnp.float32, low / len(split), high / len(split))
        factor_of = factor_of * jnp.repeat(jnp.exp(heights), dims[position] // blocks).reshape((-1,) + (1,) * (len(dims) - 1 - position))
    return factor_of


def routed_block(own_key, own, number, rows, count, top, bound, lean):
    sequence = jax.random.permutation(own_key, count)
    crowded, usual = load_shares(count, rows * top, bound, lean, True), load_shares(count, rows * top, bound, lean, False)
    places = jnp.arange(count)

    def named(lengths, turn):
        used = int((lengths > 0).sum())
        fixed = max(1, used // 4)
        moved = fixed + (places - fixed + turn * (used - fixed)) % max(1, count - fixed)
        return jnp.zeros((count,), jnp.int32).at[sequence[jnp.where(places < fixed, places, moved)]].set(jnp.asarray(lengths, jnp.int32))

    lengths = jnp.where(number % 4 == 0, named(crowded, number // 4), named(usual, number - number // 4 - 1))
    mixed = jax.random.permutation(jax.random.fold_in(own, 3), count)
    donor, taker = mixed[0:count // 2 * 2:2], mixed[1:count // 2 * 2:2]
    room = jnp.minimum(lengths[donor] - 1, bound - lengths[taker]) // 2
    room = jnp.where((donor == sequence[0]) | (taker == sequence[0]) | (lengths[taker] == 0), 0, jnp.maximum(room, 0))
    moved = jax.random.randint(jax.random.fold_in(own, 4), (count // 2,), 0, 1 << 20) % (room + 1)
    lengths = lengths.at[donor].add(-moved).at[taker].add(moved)
    labels = jnp.searchsorted(jnp.cumsum(lengths), jnp.arange(rows * top), side="right").astype(jnp.int32)
    table = labels.reshape(top, rows).T
    table = table[jax.random.permutation(jax.random.fold_in(own, 1), rows)]
    turn = jax.random.randint(jax.random.fold_in(own, 2), (rows, 1), 0, top)
    return jnp.take_along_axis(table, (jnp.arange(top)[None, :] + turn) % top, axis=1)


def load_shares(count, total, limit, skew, full):
    weights = [(1 << 20) // math.isqrt(rank ** skew) + 1 for rank in range(1, count + 1)]
    largest = limit if full else min(limit, max(-(-total // count), total * weights[0] // sum(weights)))
    least = 1 if total - largest >= count - 1 else 0
    given, spare = [largest] + [least] * (count - 1), total - largest - least * (count - 1)
    while spare > 0:
        candidates = [i for i in range(1, count) if given[i] < largest] or [i for i in range(1, count) if given[i] < limit]
        whole, left = sum([weights[i] for i in candidates]), spare
        for i in candidates:
            more = min(limit - given[i], max(1, left * weights[i] // whole), spare)
            given[i] = given[i] + more
            spare = spare - more
    return np.array(given)


def scatter_about(rng, dims, deviation, reach, cuts=(), kind=jnp.bfloat16):
    gain = block_scale(rng, dims, cuts, -0.22, 0.18) if cuts else 1.0
    values = jax.random.normal(rng, dims, jnp.float32) * deviation * gain
    return jnp.minimum(jnp.maximum(values, -reach), reach).astype(kind)


def setup_inputs(seed: int = 0) -> dict:
    seeds = jax.random.split(jax.random.key(seed), 9)
    tokens = scatter_about(seeds[0], (TOKENS, D), 1.0, 6.0, ((0, 32),))
    cotangent = scatter_about(seeds[1], (TOKENS, D), 1.0, 6.0, ((0, 32),))
    routing_keys = jax.random.split(jax.random.fold_in(seeds[2], 1), TOKENS // TOK_DEV)
    routing_turns = jax.random.permutation(jax.random.fold_in(seeds[2], 3), TOKENS // TOK_DEV)
    routing = jax.vmap(lambda own, number: routed_block(jax.random.fold_in(seeds[2], 2), own, number, TOK_DEV, EXPERTS, TOP, CAP, 2))(routing_keys, routing_turns).reshape((TOKENS, TOP))
    gate_values = jnp.clip(0.1 + 0.9 * jax.random.uniform(seeds[3], (TOKENS, TOP), jnp.float32) ** block_scale(seeds[3], (TOKENS, TOP), ((0, 32),), -0.2, 0.2), 0.1, 1.0)
    live_counts = place_ends(jax.random.randint(seeds[4], (DEVICES,), TOK_DEV // 2, TOK_DEV + 1), jax.random.fold_in(seeds[4], 1), TOK_DEV // 2, TOK_DEV).astype(jnp.int32)
    gate_weights = scatter_about(seeds[5], (EXPERTS, D, FF), D ** -0.5, 0.1875, ((0, 8), (1, 4)))
    up_weights = scatter_about(seeds[6], (EXPERTS, D, FF), D ** -0.5, 0.1875, ((0, 8), (1, 4)))
    down_weights = scatter_about(seeds[7], (EXPERTS, FF, D), FF ** -0.5, 0.3125, ((0, 8), (1, 4)))
    return {"tokens": tokens, "cotangent": cotangent, "routing": routing, "gate_values": gate_values, "live_counts": live_counts, "gate_weights": gate_weights, "up_weights": up_weights, "down_weights": down_weights}


def contract_last(left, right):
    return lax.dot_general(left, right, (((1,), (1,)), ((), ())), preferred_element_type=jnp.float32)


def contract_first(left, right):
    return lax.dot_general(left, right, (((0,), (0,)), ((), ())), preferred_element_type=jnp.float32)


def expert_rows(rows_in, grads_in, gate_w, up_w, down_w):
    pre_gate = jnp.dot(rows_in, gate_w, preferred_element_type=jnp.float32)
    pre_up = jnp.dot(rows_in, up_w, preferred_element_type=jnp.float32)
    sigmoid_gate = jax.nn.sigmoid(pre_gate)
    swish_gate = pre_gate * sigmoid_gate
    hidden = (swish_gate * pre_up).astype(jnp.bfloat16)
    outputs = jnp.dot(hidden, down_w, preferred_element_type=jnp.float32).astype(jnp.bfloat16)
    hidden_grad = contract_last(grads_in, down_w)
    gate_pre = (hidden_grad * pre_up * sigmoid_gate * (1.0 + pre_gate * (1.0 - sigmoid_gate))).astype(jnp.bfloat16)
    up_pre = (hidden_grad * swish_gate).astype(jnp.bfloat16)
    token_part = (contract_last(gate_pre, gate_w) + contract_last(up_pre, up_w)).astype(jnp.bfloat16)
    return outputs, token_part, (contract_first(rows_in, gate_pre), contract_first(rows_in, up_pre), contract_first(hidden, grads_in))


def reference(tokens, cotangent, routing, gate_values, live_counts, gate_weights, up_weights, down_weights):
    group_tok = TOK_DEV * N_EXPERT
    rows_cap = 2 * TOK_DEV * TOP
    assigned = group_tok * TOP

    def one_group(state_now, group_idx):
        row_start = group_idx * group_tok
        group_tokens = lax.dynamic_slice_in_dim(tokens, row_start, group_tok, 0)
        group_cot = lax.dynamic_slice_in_dim(cotangent, row_start, group_tok, 0)
        group_routes = lax.dynamic_slice_in_dim(routing, row_start, group_tok, 0)
        group_gates = lax.dynamic_slice_in_dim(gate_values, row_start, group_tok, 0)
        counts = lax.dynamic_slice_in_dim(live_counts, (group_idx * N_EXPERT).astype(jnp.int32), N_EXPERT, 0)
        within = jnp.arange(group_tok, dtype=jnp.int32) % TOK_DEV
        alive_rows = within < jnp.repeat(counts, TOK_DEV)
        alive_flat = jnp.repeat(alive_rows, TOP)
        target = jnp.where(alive_flat, group_routes.reshape(-1), EXPERTS).astype(jnp.int32)
        pack_order = jnp.argsort(target, stable=True).astype(jnp.int32)
        per_expert = jnp.sum((target[:, None] == jnp.arange(EXPERTS, dtype=jnp.int32)[None, :]).astype(jnp.int32), axis=0)
        starts = jnp.cumsum(per_expert) - per_expert
        tokens_pad = jnp.concatenate([group_tokens, jnp.zeros((1, D), group_tokens.dtype)], 0)
        cot_pad = jnp.concatenate([group_cot, jnp.zeros((1, D), group_cot.dtype)], 0)
        gates_pad = jnp.concatenate([group_gates.reshape(-1), jnp.zeros((1,), jnp.float32)], 0)

        def one_expert(expert_idx):
            offsets = jnp.arange(rows_cap, dtype=jnp.int32)
            valid = offsets < per_expert[expert_idx]
            picked = jnp.clip(starts[expert_idx] + offsets, 0, assigned - 1).astype(jnp.int32)
            chosen = jnp.where(valid, pack_order[picked], assigned).astype(jnp.int32)
            token_of = (chosen // TOP).astype(jnp.int32)
            rows_in = tokens_pad[token_of]
            grads_in = (gates_pad[chosen][:, None] * cot_pad[token_of].astype(jnp.float32)).astype(jnp.bfloat16)
            outputs, token_part, grads = expert_rows(rows_in, grads_in, gate_weights[expert_idx], up_weights[expert_idx], down_weights[expert_idx])
            return outputs, token_part, grads, chosen

        outputs, parts, grads, chosen = lax.map(one_expert, jnp.arange(EXPERTS, dtype=jnp.int32))
        flat_chosen = chosen.reshape(-1)
        out_assign = jnp.zeros((assigned + 1, D), outputs.dtype).at[flat_chosen].set(outputs.reshape(-1, D))[:assigned]
        part_assign = jnp.zeros((assigned + 1, D), parts.dtype).at[flat_chosen].set(parts.reshape(-1, D))[:assigned]
        expert_out = out_assign.reshape(group_tok, TOP, D).astype(jnp.float32)
        mixed = jnp.sum(group_gates[:, :, None] * expert_out, axis=1).astype(jnp.bfloat16)
        gate_grad = jnp.einsum("td,tkd->tk", group_cot.astype(jnp.float32), expert_out)
        token_grad = jnp.sum(part_assign.reshape(group_tok, TOP, D).astype(jnp.float32), axis=1).astype(jnp.bfloat16)
        rounded = tuple(lax.optimization_barrier(piece.astype(jnp.bfloat16)).astype(jnp.float32) for piece in grads)
        state_next = tuple(first + second for first, second in zip(state_now, rounded))
        return state_next, (mixed, token_grad, gate_grad)

    initial = (jnp.zeros((EXPERTS, D, FF), jnp.float32), jnp.zeros((EXPERTS, D, FF), jnp.float32), jnp.zeros((EXPERTS, FF, D), jnp.float32))
    totals, stacked = lax.scan(one_group, initial, jnp.arange(GROUPS, dtype=jnp.int32))
    mixed = stacked[0].reshape(TOKENS, D)
    token_grad = stacked[1].reshape(TOKENS, D)
    gate_grad = stacked[2].reshape(TOKENS, TOP)
    grad_gate_w = (totals[0] / GROUPS).astype(jnp.bfloat16)
    grad_up_w = (totals[1] / GROUPS).astype(jnp.bfloat16)
    grad_down_w = (totals[2] / GROUPS).astype(jnp.bfloat16)
    return (mixed, token_grad, gate_grad, grad_gate_w, grad_up_w, grad_down_w)
```

```python
import functools

import jax
import jax.numpy as jnp
from jax import lax
from jax.experimental import pallas as pl
from jax.experimental.pallas import tpu as pltpu
from jax.sharding import PartitionSpec as P

bf16, f32 = jnp.bfloat16, jnp.float32
VMEM = pl.BlockSpec(memory_space=pltpu.VMEM)
SMEM = pl.BlockSpec(memory_space=pltpu.SMEM)
SPLIT = True


def swap(value, axis, bit):
    size = lax.axis_size(axis)
    return lax.ppermute(value, axis, [(i, i ^ bit) for i in range(size)])


def nt(left, right):
    return lax.dot_general(left, right, (((1,), (1,)), ((), ())), preferred_element_type=f32)


def tn(left, right):
    return lax.dot_general(left, right, (((0,), (0,)), ((), ())), preferred_element_type=f32)


def packing(width, hidden, groups):
    rows, down_rows = width // groups, hidden // groups
    span = 2 * hidden
    rest = width - span
    folds = span // rest
    fold_rows = down_rows // folds
    assert 0 < rest <= span and span % rest == 0 and down_rows % folds == 0
    cuts = [(0, rows // 2), (rows // 2, rows)] if SPLIT else [(0, rows)]
    chunks = [
        (hi - lo, [(0, lo, 0, hi - lo, hidden, 0, 0), (1, lo, 0, hi - lo, hidden, 0, hidden)])
        for lo, hi in cuts
    ]
    down = [(2, 0, 0, down_rows, span, 0, 0)] + [
        (2, i * fold_rows, span, fold_rows, rest, down_rows, i * rest) for i in range(folds)
    ]
    return chunks + [(down_rows + fold_rows, down)]


def pack_kernel(chunks, routing, gates, live, gate_w, up_w, down_w, meta, *packed):
    tok_rows = routing.shape[1]
    top = routing.shape[0]
    alive = lax.broadcasted_iota(jnp.int32, (top, tok_rows), 1) < live[0]
    meta[...] = jnp.zeros_like(meta)
    meta[0:top, :] = jnp.where(alive, routing[...], -1).astype(f32)
    meta[top : 2 * top, :] = gates[...]
    sources = (gate_w, up_w, down_w)
    for out, (_, rects) in zip(packed, chunks):
        for src, r, c, h, w, pr, pc in rects:
            out[pr : pr + h, pc : pc + w] = sources[src][0, r : r + h, c : c + w]


def finish_kernel(chunks, groups, parts, *refs):
    n = len(chunks)
    terms, outs = refs[: n * parts], refs[n * parts :]
    for i, (_, rects) in enumerate(chunks):
        total = terms[i * parts][...].astype(f32)
        for j in range(1, parts):
            total = total + terms[i * parts + j][...].astype(f32)
        total = (total / groups).astype(bf16)
        for src, r, c, h, w, pr, pc in rects:
            outs[src][0, r : r + h, c : c + w] = total[pr : pr + h, pc : pc + w]


def expert_kernel(chunks, blocks, groups, experts, top, cap, second, *refs):
    refs = list(refs)

    def take(count):
        got = refs[:count]
        del refs[:count]
        return got

    n = len(chunks)
    metas, toks, cots = take(blocks), take(blocks), take(blocks)
    pieces = take(groups * n)
    old_m, old_g, old_s = (
        (take(blocks), take(blocks), take(blocks)) if second else ([None] * blocks,) * 3
    )
    new_m, new_g, new_s = take(blocks), take(blocks), take(blocks)
    grads = take(groups * n)
    wide, down, acc_wide, acc_down, rows_in, cots_in = refs
    tok_rows, width = toks[0].shape
    hidden_units = down.shape[0]
    me = lax.axis_index("dp")
    expert = lax.axis_index("expert")
    if second:
        expert = jnp.bitwise_xor(expert, experts // 2)
    expert = expert.astype(f32)
    bases = (width // groups, width // groups, hidden_units // groups)

    for j in range(groups):
        owner = jnp.bitwise_xor(me, j)
        for i, (_, rects) in enumerate(chunks):
            piece = pieces[j * n + i]
            for src, r, c, h, w, pr, pc in rects:
                at = pl.ds(pl.multiple_of(owner * bases[src] + r, 8), h)
                block = piece[pr : pr + h, pc : pc + w]
                if src == 2:
                    down[at, c : c + w] = block
                else:
                    wide[at, src * hidden_units + c : src * hidden_units + c + w] = block

    before = (
        lax.broadcasted_iota(jnp.int32, (tok_rows, tok_rows), 0)
        < lax.broadcasted_iota(jnp.int32, (tok_rows, tok_rows), 1)
    ).astype(bf16)
    slot = lax.broadcasted_iota(jnp.int32, (cap, tok_rows), 0)
    picks, row_gates, named = [], [], []
    for b in range(blocks):
        meta = metas[b][...]
        hits = [meta[k : k + 1, :] == expert for k in range(top)]
        gate = jnp.zeros((1, tok_rows), f32)
        mask = jnp.zeros((1, tok_rows), f32)
        for k in range(top):
            gate = jnp.where(hits[k], meta[top + k : top + k + 1, :], gate)
            mask = jnp.where(hits[k], 1.0, mask)
        ranks = jnp.dot(
            jnp.broadcast_to(mask, (8, tok_rows)).astype(bf16), before, preferred_element_type=f32
        )[0:1, :]
        place = jnp.where(mask > 0.0, ranks, -1.0).astype(jnp.int32)
        pick = slot == place
        picks.append(pick)
        named.append(hits)
        row_gates.append(jnp.sum(jnp.where(pick, gate, 0.0), axis=1, keepdims=True))
        chosen = pick.astype(bf16)
        rows_in[b * cap : (b + 1) * cap, :] = jnp.dot(
            chosen, toks[b][...], preferred_element_type=f32
        ).astype(bf16)
        cots_in[b * cap : (b + 1) * cap, :] = jnp.dot(
            chosen, cots[b][...], preferred_element_type=f32
        ).astype(bf16)

    scale = jnp.concatenate(row_gates, axis=0)
    raw_cot = cots_in[...].astype(f32)
    scaled = (scale * raw_cot).astype(bf16)
    pre = jnp.dot(rows_in[...], wide[...], preferred_element_type=f32)
    pre_gate, pre_up = pre[:, :hidden_units], pre[:, hidden_units:]
    sig = jax.nn.sigmoid(pre_gate)
    swish = pre_gate * sig
    hidden = (swish * pre_up).astype(bf16)
    hidden_grad = nt(scaled, down[...])
    gate_pre = (hidden_grad * pre_up * sig * (1.0 + pre_gate * (1.0 - sig))).astype(bf16)
    up_pre = (hidden_grad * swish).astype(bf16)
    both = jnp.concatenate([gate_pre, up_pre], axis=1)
    acc_wide[...] = tn(rows_in[...], both).astype(bf16)
    acc_down[...] = tn(hidden, scaled).astype(bf16)
    for j in range(groups):
        owner = jnp.bitwise_xor(me, j)
        for i, (_, rects) in enumerate(chunks):
            for src, r, c, h, w, pr, pc in rects:
                at = pl.ds(pl.multiple_of(owner * bases[src] + r, 8), h)
                if src == 2:
                    block = acc_down[at, c : c + w]
                else:
                    block = acc_wide[at, src * hidden_units + c : src * hidden_units + c + w]
                grads[j * n + i][pr : pr + h, pc : pc + w] = block
    outputs = jnp.dot(hidden, down[...], preferred_element_type=f32).astype(bf16).astype(f32)
    part = nt(both, wide[...]).astype(bf16)
    dots = jnp.sum(outputs * raw_cot, axis=1, keepdims=True)
    outputs = (outputs * scale).astype(bf16)
    for b in range(blocks):
        at = slice(b * cap, (b + 1) * cap)
        chosen = picks[b].astype(bf16)
        mix = tn(chosen, outputs[at])
        grad = tn(chosen, part[at])
        dot = jnp.sum(jnp.where(picks[b], dots[at], 0.0), axis=0, keepdims=True)
        if second:
            mix = mix + old_m[b][...].astype(f32)
            grad = grad + old_g[b][...].astype(f32)
        new_m[b][...] = mix.astype(bf16)
        new_g[b][...] = grad.astype(bf16)
        new_s[b][...] = jnp.zeros_like(new_s[b])
        for k in range(top):
            line = jnp.where(named[b][k], dot, 0.0)
            if second:
                line = line + old_s[b][k : k + 1, :]
            new_s[b][k : k + 1, :] = line


def add(*terms):
    total = terms[0].astype(f32)
    for term in terms[1:]:
        total = total + term.astype(f32)
    return total.astype(bf16)


def highest(value):
    return 1 << (value.bit_length() - 1)


def lowest(value):
    return value & -value


def shards(
    tokens, cotangent, routing, gate_values, live_counts, gate_weights, up_weights, down_weights
):
    experts = lax.axis_size("expert")
    groups = lax.axis_size("dp")
    tok_rows, width = tokens.shape
    top = routing.shape[1]
    hidden = gate_weights.shape[2]
    blocks = experts // 2
    mirror = experts // 2
    cap = 2 * tok_rows * top // experts
    chunks = packing(width, hidden, groups)
    n = len(chunks)
    chunk_shapes = [(rows, 2 * hidden) for rows, _ in chunks]
    meta, *packed = pl.pallas_call(
        functools.partial(pack_kernel, chunks),
        out_shape=[jax.ShapeDtypeStruct((8, tok_rows), f32)]
        + [jax.ShapeDtypeStruct(s, bf16) for s in chunk_shapes],
        in_specs=[VMEM, VMEM, SMEM, VMEM, VMEM, VMEM],
        out_specs=[VMEM] * (n + 1),
        name="pack",
    )(routing.T, gate_values.T, live_counts, gate_weights, up_weights, down_weights)

    order = sorted(range(1, blocks), key=lambda o: (o.bit_count(), o))
    metas, toks, cots = {0: meta}, {0: tokens}, {0: cotangent}
    for o in order:
        metas[o] = swap(meta, "expert", o)
    far = [swap(piece, "expert", mirror) for piece in packed]
    for o in order:
        low, high = lowest(o), highest(o)
        toks[o] = swap(toks[o ^ low], "expert", low)
        cots[o] = swap(cots[o ^ high], "expert", high)

    def spread(pieces):
        held = {0: pieces}
        bit = groups // 2
        while bit:
            for o in list(held):
                held[o | bit] = [swap(piece, "dp", bit) for piece in held[o]]
            bit //= 2
        return [piece for o in range(groups) for piece in held[o]]

    rows = blocks * cap
    flops = 2 * rows * width * hidden * 9 + 8 * blocks * cap * tok_rows * width
    line = jax.ShapeDtypeStruct((8, tok_rows), f32)
    block = jax.ShapeDtypeStruct((tok_rows, width), bf16)
    outs = (
        [block] * (2 * blocks)
        + [line] * blocks
        + [jax.ShapeDtypeStruct(s, bf16) for _ in range(groups) for s in chunk_shapes]
    )
    listed = lambda table: [table[o] for o in range(blocks)]

    def run(pieces, old):
        args = listed(metas) + listed(toks) + listed(cots) + pieces + old
        got = pl.pallas_call(
            functools.partial(
                expert_kernel, chunks, blocks, groups, experts, top, cap, bool(old)
            ),
            out_shape=outs,
            in_specs=[VMEM] * len(args),
            out_specs=[VMEM] * len(outs),
            scratch_shapes=[
                pltpu.VMEM((width, 2 * hidden), bf16),
                pltpu.VMEM((hidden, width), bf16),
                pltpu.VMEM((width, 2 * hidden), bf16),
                pltpu.VMEM((hidden, width), bf16),
                pltpu.VMEM((rows, width), bf16),
                pltpu.VMEM((rows, width), bf16),
            ],
            compiler_params=pltpu.CompilerParams(vmem_limit_bytes=60 * 1024 * 1024),
            cost_estimate=pl.CostEstimate(
                flops=flops, bytes_accessed=12 << 20, transcendentals=rows * hidden
            ),
            name="second" if old else "first",
        )(*args)
        flat = got[: 3 * blocks]
        grads = got[3 * blocks :]
        return list(flat), [grads[j * n : (j + 1) * n] for j in range(groups)]

    def gather_sums(grads):
        held = {j: grads[j] for j in range(groups)}
        terms = {j: [[piece] for piece in held[j]] for j in held}
        bit = 1
        live = list(range(groups))
        while bit < groups:
            keep = [j for j in live if not j & bit]
            for j in keep:
                away = j | bit
                sent = [
                    swap(t[0] if len(t) == 1 else add(*t), "dp", bit) for t in terms[away]
                ]
                for t, piece in zip(terms[j], sent):
                    t.append(piece)
            live = keep
            bit *= 2
        return terms[0]

    state, near_grads = run(spread(packed), [])
    near_terms = gather_sums(near_grads)
    state, far_grads = run(spread(far), state)
    mixes = {o: [state[o]] for o in range(blocks)}
    grads = {o: [state[blocks + o]] for o in range(blocks)}
    lines = state[2 * blocks :]
    line_sum = lines[0]
    for o in order:
        line_sum = line_sum + swap(lines[o], "expert", o)
    for o in reversed(order):
        low, high = lowest(o), highest(o)
        mixes[o ^ low].append(swap(add(*mixes[o]), "expert", low))
        grads[o ^ high].append(swap(add(*grads[o]), "expert", high))
    far_terms = gather_sums(far_grads)
    home = [swap(add(*terms), "expert", mirror) for terms in far_terms]
    finals = [terms + [piece] for terms, piece in zip(near_terms, home)]
    parts = len(finals[0])
    finish_in = [piece for terms in finals for piece in terms]
    weight_grads = pl.pallas_call(
        functools.partial(finish_kernel, chunks, groups, parts),
        out_shape=[
            jax.ShapeDtypeStruct(w.shape, bf16) for w in (gate_weights, up_weights, down_weights)
        ],
        in_specs=[VMEM] * len(finish_in),
        out_specs=[VMEM] * 3,
        name="finish",
    )(*finish_in)
    return (add(*mixes[0]), add(*grads[0]), line_sum[:top].T, *weight_grads)


def solution(mesh):
    rows = P(("dp", "expert"), None)
    weights = P("expert", "dp", None)
    return jax.shard_map(
        shards,
        mesh=mesh,
        in_specs=(rows, rows, rows, rows, P(("dp", "expert")), weights, weights, weights),
        out_specs=(rows, rows, rows, weights, weights, weights),
        check_vma=False,
    )
```
